512 devices in a mesh: level: 16 (over z), dev: 32 (over x, y, core).
Axes of the slice: x: 4, y: 4, z: 16, core: 2. Of those that a mesh axis runs over, the one named last changes fastest.
Arguments:
- fields: float32 [16, 512, 12, 128], P('level', 'dev'), may hold values from -6 to 6
- own_src: int32 [16, 512], P('level', 'dev'), may hold values from 0 to 15
- own_weight: bfloat16 [16, 512, 128, 128], P('level', 'dev'), may hold values from 0 to 1, as said below
- send_block: int32 [16, 32, 32, 2], P('level', 'dev'), may hold values from 0 to 15
- send_target: int32 [16, 32, 32, 2], P('level', 'dev'), may hold values from 0 to 15
- send_count: int32 [16, 32, 32], P('level', 'dev'), may hold values from 0 to 2, as said below
- send_weight: bfloat16 [16, 32, 32, 2, 128, 128], P('level', 'dev'), may hold values from 0 to 1, as said below
- left_block: int32 [16, 32, 16, 2], P('level', 'dev'), may hold values from 0 to 15
- left_target: int32 [16, 32, 16, 2], P('level', 'dev'), may hold values from 0 to 15
- left_count: int32 [16, 32, 16], P('level', 'dev'), may hold values from 0 to 2, as said below
- left_weight: bfloat16 [16, 32, 16, 2, 128, 128], P('level', 'dev'), may hold values from 0 to 1, as said below
Outputs:
- remapped: float32 [16, 512, 12, 128], P('level', 'dev')
- totals: float32 [12], replicated
The draws below stay inside these ranges and needn't reach their ends.
Inputs may be any that keep to these rules, and one draw needn't show every extreme that they name: send_count[l, s, s] = 0; for every level some receiver device gets 2 live slots from every other device of the level. left_count[m, q, m] = 0; for every device index some receiver level gets 2 live slots from every other level. `own_weight`: nonnegative; entry [k, i] is zero where old cell k and new cell i differ by more than 3; each column sums to a positive intersect fraction of at most 1. `send_weight`: nonnegative; entry [k, i] is zero where old cell k and new cell i differ by more than 3; each column sums to a positive intersect fraction of at most 1. `left_weight`: nonnegative; entry [k, i] is zero where old cell k and new cell i differ by more than 3; each column sums to a positive intersect fraction of at most 1.
All inputs are finite; a program needn't handle non-finite values.
Results may differ from the reference program's by a relative error of at most 0.0045.
Values may be sent and summed in bfloat16 or wider, within the bound.
A program may use at most 64 MiB of HBM per device.

```python
import jax
import jax.numpy as jnp
from jax import lax

COMP = 12
CELLS = 128
HALF = 3
BLK_DEV = 16
CAP = 2
LCAP = 2
PEERS = 32
LEVELS = 16
BLOCKS = 512


def band_fractions(key, lead):
    first, second, third = jax.random.split(key, 3)
    shape = lead + (CELLS, CELLS)
    rowpos = lax.broadcasted_iota(jnp.int32, shape, len(lead))
    colpos = lax.broadcasted_iota(jnp.int32, shape, len(lead) + 1)
    spread = jnp.abs(rowpos - colpos)
    middle = jax.random.uniform(first, shape, jnp.float32, 2.0, 3.0)
    beside = jax.random.uniform(second, shape, jnp.float32, 0.3, 1.0)
    raw = jnp.where(spread == 0, middle, jnp.where(spread <= HALF, beside, jnp.zeros_like(beside)))
    fraction = jax.random.uniform(third, lead + (1, CELLS), jnp.float32, 0.2, 0.8)
    return raw / jnp.sum(raw, axis=-2, keepdims=True) * fraction


def draw_own_weight(key, part):
    whole = band_fractions(jax.random.fold_in(key, 11), (LEVELS, BLOCKS))
    return whole.astype(jnp.bfloat16)


def draw_send_weight(key, part):
    whole = band_fractions(jax.random.fold_in(key, 23), (LEVELS, PEERS, PEERS, CAP))
    return whole.astype(jnp.bfloat16)


def draw_left_weight(key, part):
    whole = band_fractions(jax.random.fold_in(key, 37), (LEVELS, PEERS, LEVELS, LCAP))
    return whole.astype(jnp.bfloat16)


def draw_send_count(key, part):
    shape = (LEVELS, PEERS, PEERS)
    base = jax.random.randint(key, shape, 0, CAP + 1)
    lvl = lax.broadcasted_iota(jnp.int32, shape, 0)
    src = lax.broadcasted_iota(jnp.int32, shape, 1)
    dst = lax.broadcasted_iota(jnp.int32, shape, 2)
    heavy = (7 * lvl + 3) % PEERS
    near = ((dst - src) % PEERS == 1) | ((src - dst) % PEERS == 1)
    full = (dst == heavy) | near
    out = jnp.where(full, CAP, base)
    return jnp.where(src == dst, 0, out).astype(jnp.int32)


def draw_left_count(key, part):
    shape = (LEVELS, PEERS, LEVELS)
    base = jax.random.randint(key, shape, 0, LCAP + 1)
    src = lax.broadcasted_iota(jnp.int32, shape, 0)
    dev = lax.broadcasted_iota(jnp.int32, shape, 1)
    dst = lax.broadcasted_iota(jnp.int32, shape, 2)
    heavy = (5 * dev + 1) % LEVELS
    near = ((dst - src) % LEVELS == 1) | ((src - dst) % LEVELS == 1)
    full = (dst == heavy) | near
    out = jnp.where(full, LCAP, base)
    return jnp.where(src == dst, 0, out).astype(jnp.int32)


def with_ends(drawn, own_key, smallest, top_value):
    spot = [jax.random.randint(jax.random.fold_in(own_key, axis), (), 0, length) for axis, length in enumerate(drawn.shape)]
    widest = drawn.shape.index(max(drawn.shape))
    next_to = spot[:widest] + [(spot[widest] + 1) % drawn.shape[widest]] + spot[widest + 1:]
    return drawn.at[tuple(spot)].set(smallest).at[tuple(next_to)].set(top_value)


def block_levels(key, shape, cuts, smallest, top_value):
    def one(position, parts):
        steps = jax.random.uniform(jax.random.fold_in(jax.random.fold_in(key, 6), position), (parts,), jnp.float32, smallest / len(cuts), top_value / len(cuts))
        return jnp.repeat(jnp.exp(steps), shape[position] // parts).reshape((-1,) + (1,) * (len(shape) - position - 1))

    loudness = one(*cuts[0])
    for cut in cuts[1:]:
        loudness = loudness * one(*cut)
    return loudness


def centred(rng, dims, deviation, reach, cuts=(), dtype=jnp.bfloat16):
    result = deviation * jax.random.normal(rng, dims, jnp.float32)
    if cuts:
        result = result * block_levels(rng, dims, cuts, -0.22, 0.18)
    return jnp.clip(result, -reach, reach).astype(dtype)


def setup_inputs(seed: int = 0) -> dict:
    splits = jax.random.split(jax.random.key(seed), 12)
    fields = centred(splits[0], (LEVELS, BLOCKS, COMP, CELLS), 1.0, 6.0, ((0, 16), (1, 32)), jnp.float32)
    own_src = with_ends(jax.random.randint(splits[1], (LEVELS, BLOCKS), 0, BLK_DEV), jax.random.fold_in(splits[1], 1), 0, BLK_DEV - 1).astype(jnp.int32)
    own_weight = draw_own_weight(jax.random.fold_in(splits[11], 71), 0)
    send_block = with_ends(jax.random.randint(splits[3], (LEVELS, PEERS, PEERS, CAP), 0, BLK_DEV), jax.random.fold_in(splits[3], 1), 0, BLK_DEV - 1).astype(jnp.int32)
    send_target = with_ends(jax.random.randint(splits[4], (LEVELS, PEERS, PEERS, CAP), 0, BLK_DEV), jax.random.fold_in(splits[4], 1), 0, BLK_DEV - 1).astype(jnp.int32)
    send_count = draw_send_count(jax.random.fold_in(splits[11], 71), 0)
    send_weight = draw_send_weight(jax.random.fold_in(splits[11], 71), 0)
    left_block = with_ends(jax.random.randint(splits[7], (LEVELS, PEERS, LEVELS, LCAP), 0, BLK_DEV), jax.random.fold_in(splits[7], 1), 0, BLK_DEV - 1).astype(jnp.int32)
    left_target = with_ends(jax.random.randint(splits[8], (LEVELS, PEERS, LEVELS, LCAP), 0, BLK_DEV), jax.random.fold_in(splits[8], 1), 0, BLK_DEV - 1).astype(jnp.int32)
    left_count = draw_left_count(jax.random.fold_in(splits[11], 71), 0)
    left_weight = draw_left_weight(jax.random.fold_in(splits[11], 71), 0)
    return dict(fields=fields, own_src=own_src, own_weight=own_weight, send_block=send_block, send_target=send_target, send_count=send_count, send_weight=send_weight, left_block=left_block, left_target=left_target, left_count=left_count, left_weight=left_weight)


def reference(fields, own_src, own_weight, send_block, send_target, send_count, send_weight, left_block, left_target, left_count, left_weight):
    levels = fields.shape[0]
    peers = send_count.shape[1]
    blocks = fields.shape[1] // peers
    comp = fields.shape[2]
    cells = fields.shape[3]
    rounded = fields.astype(jnp.bfloat16).reshape(levels, peers, blocks, comp, cells)
    highest = lax.Precision.HIGHEST

    own_index = own_src.reshape(levels, peers, blocks, 1, 1).astype(jnp.int32)
    own_donor = jnp.take_along_axis(rounded, own_index, axis=2).astype(jnp.float32)
    own_frac = own_weight.reshape(levels, peers, blocks, cells, cells).astype(jnp.float32)
    own = jnp.einsum("lqbmk,lqbki->lqbmi", own_donor, own_frac, precision=highest)

    source_dev = lax.broadcasted_iota(jnp.int32, (peers, 1, 1), 0)
    recv_dev = lax.broadcasted_iota(jnp.int32, (1, peers, 1), 1)
    slot_cap = send_block.shape[3]

    def level_intra(packed):
        flds, blk, tgt, cnt, wts = packed
        donors = flds[source_dev, blk]
        valid = lax.broadcasted_iota(jnp.int32, (1, 1, slot_cap), 2) < cnt[:, :, None]
        donors = jnp.where(valid[..., None, None], donors, jnp.zeros_like(donors))
        contrib = jnp.einsum("spcmk,spcki->spcmi", donors.astype(jnp.float32), wts.astype(jnp.float32), precision=highest)
        receive = (recv_dev * blocks + tgt).reshape(-1).astype(jnp.int32)
        total = jnp.zeros((peers * blocks, comp, cells), jnp.float32)
        return total.at[receive].add(contrib.reshape(-1, comp, cells)).reshape(peers, blocks, comp, cells)

    intra = lax.map(level_intra, (rounded, send_block, send_target, send_count, send_weight))

    left_cap = left_block.shape[3]
    dev_index = lax.broadcasted_iota(jnp.int32, (peers, 1, 1), 0)

    def level_left(packed):
        flds, blk, cnt, wts = packed
        donors = flds[dev_index, blk]
        valid = lax.broadcasted_iota(jnp.int32, (1, 1, left_cap), 2) < cnt[:, :, None]
        donors = jnp.where(valid[..., None, None], donors, jnp.zeros_like(donors))
        return jnp.einsum("qlcmk,qlcki->qlcmi", donors.astype(jnp.float32), wts.astype(jnp.float32), precision=highest)

    left_terms = lax.map(level_left, (rounded, left_block, left_count, left_weight))
    dst_level = lax.broadcasted_iota(jnp.int32, (1, 1, levels, 1), 2)
    dev_here = lax.broadcasted_iota(jnp.int32, (1, peers, 1, 1), 1)
    recv_left = ((dst_level * peers + dev_here) * blocks + left_target).reshape(-1).astype(jnp.int32)
    leftover = jnp.zeros((levels * peers * blocks, comp, cells), jnp.float32)
    leftover = leftover.at[recv_left].add(left_terms.reshape(-1, comp, cells))
    leftover = leftover.reshape(levels, peers, blocks, comp, cells)

    remapped = (own + intra + leftover).reshape(levels, peers * blocks, comp, cells)
    totals = jnp.sum(remapped, axis=(0, 1, 3)) / (CELLS * BLK_DEV)
    return remapped, totals
```

```python
import functools

import jax
import jax.numpy as jnp
from jax import lax
from jax.experimental import pallas as pl
from jax.experimental.pallas import tpu as pltpu
from jax.sharding import PartitionSpec as P

MESH = pl.DeviceIdType.MESH
F32 = jnp.float32
BF16 = jnp.bfloat16
ROWS = 16


def kernel(
    nd,
    nl,
    comp,
    own_src_hbm,
    send_block_hbm,
    send_target_hbm,
    send_count_hbm,
    left_block_hbm,
    left_target_hbm,
    left_count_hbm,
    fields_hbm,
    own_hbm,
    send_hbm,
    left_hbm,
    out_ref,
    tot_ref,
    own_src,
    send_block,
    send_target,
    send_count,
    left_block,
    left_target,
    left_count,
    fields,
    own_w,
    send_w,
    left_w,
    load_sem,
    rounded,
    own_acc,
    sbuf,
    rbuf,
    lsbuf,
    lrbuf,
    trow,
    urow,
    go_lvl,
    send_sem,
    recv_sem,
):
    dev = lax.axis_index("dev")
    lvl = lax.axis_index("level")
    blocks, cells = own_w.shape[:2]
    cap = send_w.shape[1]
    lcap = left_w.shape[1]

    tables = [
        (left_block_hbm, left_block),
        (left_count_hbm, left_count),
        (left_target_hbm, left_target),
        (send_block_hbm, send_block),
        (send_count_hbm, send_count),
        (send_target_hbm, send_target),
        (own_src_hbm, own_src),
        (fields_hbm, fields),
    ]
    table_loads = [pltpu.make_async_copy(src, dst, load_sem.at[0]) for src, dst in tables]
    left_load = pltpu.make_async_copy(left_hbm, left_w, load_sem.at[1])
    send_load = pltpu.make_async_copy(send_hbm, send_w, load_sem.at[2])
    own_load = pltpu.make_async_copy(own_hbm, own_w, load_sem.at[3])
    for load in [*table_loads, left_load, send_load, own_load]:
        load.start()

    barrier = pltpu.get_barrier_semaphore()

    def at_dev(p):
        return {"dev": p, "level": lvl}

    def at_lvl(p):
        return {"dev": dev, "level": p}

    def other_devs(step):
        pl.loop(0, dev)(step)
        pl.loop(dev + 1, nd)(step)

    @other_devs
    def _(p):
        pl.semaphore_signal(barrier, inc=1, device_id=at_dev(p), device_id_type=MESH)

    @pl.loop(lvl + 1, nl)
    def _(p):
        pl.semaphore_signal(barrier, inc=1, device_id=at_lvl(p), device_id_type=MESH)

    zero = jnp.zeros((2 * ROWS, cells), BF16)
    rbuf[dev] = zero
    lrbuf[lvl] = zero

    for load in table_loads:
        load.wait()

    pad = jnp.zeros((ROWS - comp, cells), F32)
    for b in range(blocks):
        block = fields[pl.ds(b, comp, stride=blocks), :]
        rounded[b] = jnp.concatenate([block, pad], axis=0).astype(BF16)
    rounded[blocks] = jnp.zeros((ROWS, cells), BF16)

    row_id = lax.broadcasted_iota(jnp.int32, (ROWS, cells), 0)

    def product(index, weight):
        return jnp.dot(rounded[index], weight, preferred_element_type=F32)

    def message(buf, p, c, slot_block, slot_target, slot_count, weights):
        index = jnp.where(c < slot_count[0, p], slot_block[c, p], blocks)
        term = product(index, weights[p, c])
        target = slot_target[c, p].astype(F32)
        buf[p, c * ROWS : (c + 1) * ROWS, :] = jnp.where(row_id == comp, target, term).astype(BF16)
        return term

    part = jnp.zeros((ROWS, cells), F32)
    left_load.wait()
    for p in range(nl):
        for c in range(lcap):
            part += message(lsbuf, p, c, left_block, left_target, left_count, left_w)
    send_load.wait()
    own_load.wait()
    for p in range(nd):
        for c in range(cap):
            part += message(sbuf, p, c, send_block, send_target, send_count, send_w)
    for b in range(blocks):
        term = product(own_src[0, b], own_w[b])
        part += term
        own_acc[b] = term

    sums = jnp.sum(part, axis=1, keepdims=True)
    same = row_id == lax.broadcasted_iota(jnp.int32, (ROWS, cells), 1)
    row = jnp.sum(jnp.where(same, sums, 0.0), axis=0, keepdims=True)
    trow[dev] = row

    def send(src, dst, k, who):
        pltpu.make_async_remote_copy(
            src_ref=src, dst_ref=dst, send_sem=send_sem.at[k], recv_sem=recv_sem.at[k], device_id=who, device_id_type=MESH
        ).start()

    pl.semaphore_wait(barrier, nd - 1 + lvl)

    @other_devs
    def _(p):
        send(trow.at[dev], trow.at[dev], 0, at_dev(p))

    @pl.loop(0, lvl)
    def _(p):
        send(lsbuf.at[p], lrbuf.at[lvl], 1, at_lvl(p))

    @pl.loop(0, lvl)
    def _(p):
        pl.semaphore_signal(go_lvl, inc=1, device_id=at_lvl(p), device_id_type=MESH)

    def wait_recv(buf, n, k):
        ref = buf.at[pl.ds(0, n - 1)]
        pltpu.make_async_copy(ref, ref, recv_sem.at[k]).wait()

    def wait_send(buf, n, k):
        ref = buf.at[pl.ds(0, n - 1)]
        pltpu.make_async_copy(ref, ref, send_sem.at[k]).wait()

    def total(ref, n):
        terms = [ref[i] for i in range(n)]
        while len(terms) > 1:
            half = len(terms) // 2
            terms = [a + b for a, b in zip(terms[:half], terms[half:])] + terms[2 * half :]
        return terms[0]

    wait_recv(trow, nd, 0)
    urow[lvl] = total(trow, nd)

    @pl.loop(0, lvl)
    def _(p):
        send(urow.at[lvl], urow.at[lvl], 3, at_lvl(p))

    def place(buf, acc, p, slots):
        for c in range(slots):
            got = buf[p, c * ROWS : (c + 1) * ROWS, :].astype(F32)
            target = jnp.broadcast_to(got[comp : comp + 1], (ROWS, cells))
            acc = [a + jnp.where(target == float(b), got, 0.0) for b, a in enumerate(acc)]
        return acc

    @other_devs
    def _(p):
        send(sbuf.at[p], rbuf.at[dev], 2, at_dev(p))

    @pl.when(lvl < nl - 1)
    def _():
        pl.semaphore_wait(go_lvl, nl - 1 - lvl)

    @pl.loop(lvl + 1, nl)
    def _(p):
        send(urow.at[lvl], urow.at[lvl], 3, at_lvl(p))

    @pl.loop(lvl + 1, nl)
    def _(p):
        send(lsbuf.at[p], lrbuf.at[lvl], 1, at_lvl(p))

    acc = [own_acc[b] for b in range(blocks)]
    wait_recv(rbuf, nd, 2)
    acc = lax.fori_loop(0, nd, lambda p, a: place(rbuf, a, p, cap), acc)
    wait_recv(lrbuf, nl, 1)
    acc = lax.fori_loop(0, nl, lambda p, a: place(lrbuf, a, p, lcap), acc)
    for b in range(blocks):
        out_ref[pl.ds(b, comp, stride=blocks), :] = acc[b][:comp]
    wait_send(trow, nd, 0)
    wait_send(lsbuf, nl, 1)
    wait_send(sbuf, nd, 2)
    wait_send(urow, nl, 3)
    wait_recv(urow, nl, 3)
    tot_ref[...] = (total(urow, nl) / (cells * blocks))[0, :comp]


def solution(mesh):
    nd = mesh.shape["dev"]
    nl = mesh.shape["level"]

    def body(
        fields,
        own_src,
        own_weight,
        send_block,
        send_target,
        send_count,
        send_weight,
        left_block,
        left_target,
        left_count,
        left_weight,
    ):
        blocks, comp, cells = fields.shape[1:]
        cap = send_weight.shape[3]
        lcap = left_weight.shape[3]
        smem = functools.partial(pltpu.SMEM, dtype=jnp.int32)
        hbm = pl.BlockSpec(memory_space=pl.ANY)
        vmem = pl.BlockSpec(memory_space=pltpu.VMEM)
        dma = pltpu.SemaphoreType.DMA
        remapped, totals = pl.pallas_call(
            functools.partial(kernel, nd, nl, comp),
            out_shape=(
                pltpu.VMEM((comp * blocks, cells), F32),
                pltpu.VMEM((comp,), F32),
            ),
            in_specs=[hbm] * 11,
            out_specs=(vmem, vmem),
            scratch_shapes=[
                smem((1, blocks)),
                smem((cap, nd)),
                smem((cap, nd)),
                smem((1, nd)),
                smem((lcap, nl)),
                smem((lcap, nl)),
                smem((1, nl)),
                pltpu.VMEM((comp * blocks, cells), F32),
                pltpu.VMEM((blocks, cells, cells), BF16),
                pltpu.VMEM((nd, cap, cells, cells), BF16),
                pltpu.VMEM((nl, lcap, cells, cells), BF16),
                dma((4,)),
                pltpu.VMEM((blocks + 1, ROWS, cells), BF16),
                pltpu.VMEM((blocks, ROWS, cells), F32),
                pltpu.VMEM((nd, cap * ROWS, cells), BF16),
                pltpu.VMEM((nd, cap * ROWS, cells), BF16),
                pltpu.VMEM((nl, lcap * ROWS, cells), BF16),
                pltpu.VMEM((nl, lcap * ROWS, cells), BF16),
                pltpu.VMEM((nd, 1, cells), F32),
                pltpu.VMEM((nl, 1, cells), F32),
                pltpu.SemaphoreType.REGULAR,
                dma((4,)),
                dma((4,)),
            ],
            compiler_params=pltpu.CompilerParams(collective_id=0, has_side_effects=True),
        )(
            own_src,
            send_block[0, 0].T,
            send_target[0, 0].T,
            send_count[0],
            left_block[0, 0].T,
            left_target[0, 0].T,
            left_count[0],
            fields[0].transpose(1, 0, 2).reshape(comp * blocks, cells),
            own_weight[0],
            send_weight[0, 0],
            left_weight[0, 0],
        )
        remapped = remapped.reshape(comp, blocks, cells).transpose(1, 0, 2)
        return remapped[None], totals

    in_specs = (
        P("level", "dev", None, None),
        P("level", "dev"),
        P("level", "dev", None, None),
        P("level", "dev", None, None),
        P("level", "dev", None, None),
        P("level", "dev", None),
        P("level", "dev", None, None, None, None),
        P("level", "dev", None, None),
        P("level", "dev", None, None),
        P("level", "dev", None),
        P("level", "dev", None, None, None, None),
    )
    out_specs = (P("level", "dev", None, None), P())
    return jax.shard_map(body, mesh=mesh, in_specs=in_specs, out_specs=out_specs, check_vma=False)
```

```python
import functools

import jax
import jax.numpy as jnp
from jax import lax
from jax.experimental import pallas as pl
from jax.experimental.pallas import tpu as pltpu
from jax.sharding import PartitionSpec as P

MESH = pl.DeviceIdType.MESH
F32 = jnp.float32
BF16 = jnp.bfloat16
ROWS = 16
PIECES = 4


def kernel(
    nd,
    nl,
    comp,
    own_src_hbm,
    send_block_hbm,
    send_target_hbm,
    send_count_hbm,
    left_block_hbm,
    left_target_hbm,
    left_count_hbm,
    fields_hbm,
    own_hbm,
    send_hbm,
    left_hbm,
    out_ref,
    tot_ref,
    own_src,
    send_block,
    send_target,
    send_count,
    left_block,
    left_target,
    left_count,
    fields,
    own_w,
    send_w,
    left_w,
    load_sem,
    rounded,
    own_acc,
    sbuf,
    rbuf,
    lsbuf,
    lrbuf,
    trow,
    urow,
    go_lvl,
    send_sem,
    recv_sem,
):
    dev = lax.axis_index("dev")
    lvl = lax.axis_index("level")
    blocks, cells = own_w.shape[:2]
    cap = send_w.shape[1]
    lcap = left_w.shape[1]

    tables = [
        (left_block_hbm, left_block),
        (left_count_hbm, left_count),
        (left_target_hbm, left_target),
        (send_block_hbm, send_block),
        (send_count_hbm, send_count),
        (send_target_hbm, send_target),
        (own_src_hbm, own_src),
        (fields_hbm, fields),
    ]
    table_loads = [pltpu.make_async_copy(src, dst, load_sem.at[0]) for src, dst in tables]
    half = nd // 2

    def pieces(src, dst, lo, hi, n, k):
        size = (hi - lo) // n
        return [
            pltpu.make_async_copy(
                src.at[lo + i * size : lo + (i + 1) * size], dst.at[lo + i * size : lo + (i + 1) * size], load_sem.at[k]
            )
            for i in range(n)
        ]

    left_load = pieces(left_hbm, left_w, 0, nl, PIECES, 1)
    first_load = pieces(send_hbm, send_w, 0, half, PIECES, 2)
    second_load = pieces(send_hbm, send_w, half, nd, PIECES, 3)
    own_load = pieces(own_hbm, own_w, 0, blocks, PIECES // 2, 4)
    for load in [*table_loads, *left_load, *first_load, *second_load, *own_load]:
        load.start()

    barrier = pltpu.get_barrier_semaphore()

    def at_dev(p):
        return {"dev": p, "level": lvl}

    def at_lvl(p):
        return {"dev": dev, "level": p}

    def other_devs(step):
        pl.loop(0, dev)(step)
        pl.loop(dev + 1, nd)(step)

    @other_devs
    def _(p):
        pl.semaphore_signal(barrier, inc=1, device_id=at_dev(p), device_id_type=MESH)

    summing = dev % 2 == 1
    partner = dev + 1 - 2 * (dev % 2)

    def at_partner(p):
        return {"dev": partner, "level": p}

    @pl.loop(lvl + 1, nl)
    def _(p):
        pl.semaphore_signal(barrier, inc=1, device_id=at_lvl(p), device_id_type=MESH)

    @pl.when(jnp.logical_not(summing))
    def _():
        @pl.loop(lvl + 1, nl)
        def _(p):
            pl.semaphore_signal(barrier, inc=1, device_id=at_partner(p), device_id_type=MESH)

    zero = jnp.zeros((2 * ROWS, cells), BF16)
    rbuf[dev] = zero
    lrbuf[lvl] = zero

    for load in table_loads:
        load.wait()

    pad = jnp.zeros((ROWS - comp, cells), F32)
    for b in range(blocks):
        block = fields[pl.ds(b, comp, stride=blocks), :]
        rounded[b] = jnp.concatenate([block, pad], axis=0).astype(BF16)
    rounded[blocks] = jnp.zeros((ROWS, cells), BF16)

    row_id = lax.broadcasted_iota(jnp.int32, (ROWS, cells), 0)

    def product(index, weight):
        return jnp.dot(rounded[index], weight, preferred_element_type=F32)

    def message(buf, p, c, slot_block, slot_target, slot_count, weights):
        index = jnp.where(c < slot_count[0, p], slot_block[c, p], blocks)
        term = product(index, weights[p, c])
        target = slot_target[c, p].astype(F32)
        buf[p, c * ROWS : (c + 1) * ROWS, :] = jnp.where(row_id == comp, target, term).astype(BF16)
        return term

    part = jnp.zeros((ROWS, cells), F32)
    for load in left_load:
        load.wait()
    for p in range(nl):
        for c in range(lcap):
            part += message(lsbuf, p, c, left_block, left_target, left_count, left_w)
    for load in first_load:
        load.wait()
    for p in range(half):
        for c in range(cap):
            part += message(sbuf, p, c, send_block, send_target, send_count, send_w)
    for load in second_load:
        load.wait()
    for load in own_load:
        load.wait()
    for p in range(half, nd):
        for c in range(cap):
            part += message(sbuf, p, c, send_block, send_target, send_count, send_w)
    for b in range(blocks):
        term = product(own_src[0, b], own_w[b])
        part += term
        own_acc[b] = term

    sums = jnp.sum(part, axis=1, keepdims=True)
    same = row_id == lax.broadcasted_iota(jnp.int32, (ROWS, cells), 1)
    row = jnp.sum(jnp.where(same, sums, 0.0), axis=0, keepdims=True)
    trow[dev] = row

    def send(src, dst, k, who):
        pltpu.make_async_remote_copy(
            src_ref=src, dst_ref=dst, send_sem=send_sem.at[k], recv_sem=recv_sem.at[k], device_id=who, device_id_type=MESH
        ).start()

    pl.semaphore_wait(barrier, nd - 1 + lvl + lvl * (dev % 2))

    @pl.loop(0, lvl)
    def _(p):
        pl.semaphore_signal(go_lvl, inc=1, device_id=at_lvl(p), device_id_type=MESH)

    def report(i):
        send(trow.at[dev], trow.at[dev], 0, at_dev(2 * i + 1))

    pl.loop(0, dev // 2)(report)
    pl.loop((dev + 1) // 2, nd // 2)(report)

    @pl.loop(0, lvl)
    def _(p):
        send(lsbuf.at[p], lrbuf.at[lvl], 1, at_lvl(p))

    def wait_recv(buf, n, k):
        ref = buf.at[pl.ds(0, n - 1)]
        pltpu.make_async_copy(ref, ref, recv_sem.at[k]).wait()

    def wait_send(buf, n, k):
        ref = buf.at[pl.ds(0, n - 1)]
        pltpu.make_async_copy(ref, ref, send_sem.at[k]).wait()

    def total(ref, n):
        terms = [ref[i] for i in range(n)]
        while len(terms) > 1:
            half = len(terms) // 2
            terms = [a + b for a, b in zip(terms[:half], terms[half:])] + terms[2 * half :]
        return terms[0]

    def tell(p):
        send(urow.at[lvl], urow.at[lvl], 3, at_lvl(p))
        send(urow.at[lvl], urow.at[lvl], 3, at_partner(p))

    @pl.when(summing)
    def _():
        wait_recv(trow, nd, 0)
        urow[lvl] = total(trow, nd)
        pl.loop(0, lvl)(tell)
        send(urow.at[lvl], urow.at[lvl], 3, at_partner(lvl))

    def place(buf, acc, p, slots):
        for c in range(slots):
            got = buf[p, c * ROWS : (c + 1) * ROWS, :].astype(F32)
            target = jnp.broadcast_to(got[comp : comp + 1], (ROWS, cells))
            acc = [a + jnp.where(target == float(b), got, 0.0) for b, a in enumerate(acc)]
        return acc

    @other_devs
    def _(p):
        send(sbuf.at[p], rbuf.at[dev], 2, at_dev(p))

    @pl.when(lvl < nl - 1)
    def _():
        pl.semaphore_wait(go_lvl, nl - 1 - lvl)

    @pl.loop(lvl + 1, nl)
    def _(p):
        send(lsbuf.at[p], lrbuf.at[lvl], 1, at_lvl(p))

    @pl.when(summing)
    def _():
        pl.loop(lvl + 1, nl)(tell)

    acc = [own_acc[b] for b in range(blocks)]
    wait_recv(rbuf, nd, 2)
    acc = lax.fori_loop(0, nd, lambda p, a: place(rbuf, a, p, cap), acc)
    wait_recv(lrbuf, nl, 1)
    acc = lax.fori_loop(0, nl, lambda p, a: place(lrbuf, a, p, lcap), acc)
    for b in range(blocks):
        out_ref[pl.ds(b, comp, stride=blocks), :] = acc[b][:comp]
    wait_send(lsbuf, nl, 1)
    wait_send(sbuf, nd, 2)

    @pl.when(summing)
    def _():
        wait_send(trow, nd // 2, 0)
        wait_send(trow, 2 * nl, 3)
        wait_recv(urow, nl, 3)

    @pl.when(jnp.logical_not(summing))
    def _():
        wait_send(trow, nd // 2 + 1, 0)
        wait_recv(urow, nl + 1, 3)

    tot_ref[...] = (total(urow, nl) / (cells * blocks))[0, :comp]


def deliver(blocks_in, totals_in, blocks_out, totals_out, sem):
    copies = [
        pltpu.make_async_copy(blocks_in, blocks_out, sem.at[0]),
        pltpu.make_async_copy(totals_in, totals_out, sem.at[1]),
    ]
    for copy in copies:
        copy.start()
    for copy in copies:
        copy.wait()


def solution(mesh):
    nd = mesh.shape["dev"]
    nl = mesh.shape["level"]

    def body(
        fields,
        own_src,
        own_weight,
        send_block,
        send_target,
        send_count,
        send_weight,
        left_block,
        left_target,
        left_count,
        left_weight,
    ):
        blocks, comp, cells = fields.shape[1:]
        cap = send_weight.shape[3]
        lcap = left_weight.shape[3]
        smem = functools.partial(pltpu.SMEM, dtype=jnp.int32)
        hbm = pl.BlockSpec(memory_space=pl.ANY)
        vmem = pl.BlockSpec(memory_space=pltpu.VMEM)
        dma = pltpu.SemaphoreType.DMA
        remapped, totals = pl.pallas_call(
            functools.partial(kernel, nd, nl, comp),
            out_shape=(
                pltpu.VMEM((comp * blocks, cells), F32),
                pltpu.VMEM((comp,), F32),
            ),
            in_specs=[hbm] * 11,
            out_specs=(vmem, vmem),
            scratch_shapes=[
                smem((1, blocks)),
                smem((cap, nd)),
                smem((cap, nd)),
                smem((1, nd)),
                smem((lcap, nl)),
                smem((lcap, nl)),
                smem((1, nl)),
                pltpu.VMEM((comp * blocks, cells), F32),
                pltpu.VMEM((blocks, cells, cells), BF16),
                pltpu.VMEM((nd, cap, cells, cells), BF16),
                pltpu.VMEM((nl, lcap, cells, cells), BF16),
                dma((5,)),
                pltpu.VMEM((blocks + 1, ROWS, cells), BF16),
                pltpu.VMEM((blocks, ROWS, cells), F32),
                pltpu.VMEM((nd, cap * ROWS, cells), BF16),
                pltpu.VMEM((nd, cap * ROWS, cells), BF16),
                pltpu.VMEM((nl, lcap * ROWS, cells), BF16),
                pltpu.VMEM((nl, lcap * ROWS, cells), BF16),
                pltpu.VMEM((nd, 1, cells), F32),
                pltpu.VMEM((nl, 1, cells), F32),
                pltpu.SemaphoreType.REGULAR,
                dma((4,)),
                dma((4,)),
            ],
            compiler_params=pltpu.CompilerParams(collective_id=0, has_side_effects=True),
        )(
            own_src,
            send_block[0, 0].T,
            send_target[0, 0].T,
            send_count[0],
            left_block[0, 0].T,
            left_target[0, 0].T,
            left_count[0],
            fields[0].transpose(1, 0, 2).reshape(comp * blocks, cells),
            own_weight[0],
            send_weight[0, 0],
            left_weight[0, 0],
        )
        remapped, totals = pl.pallas_call(
            deliver,
            out_shape=(
                jax.ShapeDtypeStruct((comp * blocks, cells), F32),
                jax.ShapeDtypeStruct((comp,), F32),
            ),
            in_specs=[vmem] * 2,
            out_specs=(hbm, hbm),
            scratch_shapes=[dma((2,))],
            compiler_params=pltpu.CompilerParams(vmem_limit_bytes=1 << 20),
        )(pltpu.with_memory_space_constraint(remapped, pltpu.VMEM), pltpu.with_memory_space_constraint(totals, pltpu.VMEM))
        remapped = remapped.reshape(comp, blocks, cells).transpose(1, 0, 2)
        return remapped[None], totals

    in_specs = (
        P("level", "dev", None, None),
        P("level", "dev"),
        P("level", "dev", None, None),
        P("level", "dev", None, None),
        P("level", "dev", None, None),
        P("level", "dev", None),
        P("level", "dev", None, None, None, None),
        P("level", "dev", None, None),
        P("level", "dev", None, None),
        P("level", "dev", None),
        P("level", "dev", None, None, None, None),
    )
    out_specs = (P("level", "dev", None, None), P())
    return jax.shard_map(body, mesh=mesh, in_specs=in_specs, out_specs=out_specs, check_vma=False)
```

```python
import functools

import jax
import jax.numpy as jnp
from jax import lax
from jax.experimental import pallas as pl
from jax.experimental.pallas import tpu as pltpu
from jax.sharding import PartitionSpec as P

MESH = pl.DeviceIdType.MESH
F32 = jnp.float32
BF16 = jnp.bfloat16
ROWS = 16
HALF = 8
PACKED = 24
PIECES = 4


def kernel(
    nd,
    nl,
    comp,
    own_src_hbm,
    send_block_hbm,
    send_target_hbm,
    send_count_hbm,
    left_block_hbm,
    left_target_hbm,
    left_count_hbm,
    fields_hbm,
    own_hbm,
    send_hbm,
    left_hbm,
    out_ref,
    tot_ref,
    own_src,
    send_block,
    send_target,
    send_count,
    left_block,
    left_count,
    fields,
    own_w,
    send_w,
    left_w,
    load_sem,
    rounded,
    own_acc,
    sbuf,
    rbuf,
    lsbuf,
    lrbuf,
    trow,
    urow,
    every,
    places,
    targets,
    go_lvl,
    send_sem,
    recv_sem,
):
    dev = lax.axis_index("dev")
    lvl = lax.axis_index("level")
    blocks, cells = own_w.shape[:2]
    cap = send_w.shape[1]
    lcap = left_w.shape[1]

    tables = [
        (left_block_hbm, left_block),
        (left_count_hbm, left_count),
        (send_block_hbm, send_block),
        (send_count_hbm, send_count),
        (send_target_hbm, send_target),
        (own_src_hbm, own_src),
        (fields_hbm, fields),
        (left_target_hbm, places.at[lvl]),
    ]
    table_loads = [pltpu.make_async_copy(src, dst, load_sem.at[0]) for src, dst in tables]
    half = nd // 2

    def pieces(src, dst, lo, hi, n, k):
        size = (hi - lo) // n
        return [
            pltpu.make_async_copy(
                src.at[lo + i * size : lo + (i + 1) * size], dst.at[lo + i * size : lo + (i + 1) * size], load_sem.at[k]
            )
            for i in range(n)
        ]

    left_load = pieces(left_hbm, left_w, 0, nl, PIECES, 1)
    first_load = pieces(send_hbm, send_w, 0, half, PIECES, 2)
    second_load = pieces(send_hbm, send_w, half, nd, PIECES, 3)
    own_load = pieces(own_hbm, own_w, 0, blocks, PIECES // 2, 4)
    for load in [*table_loads, *left_load, *first_load, *second_load, *own_load]:
        load.start()

    barrier = pltpu.get_barrier_semaphore()

    def at_dev(p):
        return {"dev": p, "level": lvl}

    def at_lvl(p):
        return {"dev": dev, "level": p}

    def other_devs(step):
        pl.loop(0, dev)(step)
        pl.loop(dev + 1, nd)(step)

    @other_devs
    def _(p):
        pl.semaphore_signal(barrier, inc=1, device_id=at_dev(p), device_id_type=MESH)

    summing = dev % 2 == 1
    partner = dev + 1 - 2 * (dev % 2)

    def at_partner(p):
        return {"dev": partner, "level": p}

    @pl.loop(lvl + 1, nl)
    def _(p):
        pl.semaphore_signal(barrier, inc=1, device_id=at_lvl(p), device_id_type=MESH)

    @pl.when(jnp.logical_not(summing))
    def _():
        @pl.loop(lvl + 1, nl)
        def _(p):
            pl.semaphore_signal(barrier, inc=1, device_id=at_partner(p), device_id_type=MESH)

    first_dev, first_lvl = 1, 0
    is_first = jnp.logical_and(dev == first_dev, lvl == first_lvl)
    is_far = jnp.logical_and(dev != first_dev, lvl != first_lvl)

    @pl.when(is_first)
    def _():
        @pl.loop(1, nl)
        def _(l):
            def greet(p):
                pl.semaphore_signal(barrier, inc=1, device_id={"dev": p, "level": l}, device_id_type=MESH)

            pl.loop(0, first_dev)(greet)
            pl.loop(first_dev + 1, nd)(greet)

    zero = jnp.zeros((2 * ROWS, cells), BF16)
    rbuf[dev] = zero
    lrbuf[lvl, :PACKED] = zero[:PACKED]

    for load in table_loads:
        load.wait()

    pad = jnp.zeros((ROWS - comp, cells), F32)
    for b in range(blocks):
        block = fields[pl.ds(b, comp, stride=blocks), :]
        rounded[b] = jnp.concatenate([block, pad], axis=0).astype(BF16)
    rounded[blocks] = jnp.zeros((ROWS, cells), BF16)

    row_id = lax.broadcasted_iota(jnp.int32, (ROWS, cells), 0)

    def product(index, weight):
        return jnp.dot(rounded[index], weight, preferred_element_type=F32)

    def message(buf, p, c, slot_block, slot_target, slot_count, weights):
        index = jnp.where(c < slot_count[0, p], slot_block[c, p], blocks)
        term = product(index, weights[p, c])
        target = slot_target[c, p].astype(F32)
        buf[p, c * ROWS : (c + 1) * ROWS, :] = jnp.where(row_id == comp, target, term).astype(BF16)
        return term

    part = jnp.zeros((ROWS, cells), F32)
    for load in left_load:
        load.wait()
    for p in range(nl):
        terms = [
            product(jnp.where(c < left_count[0, p], left_block[c, p], blocks), left_w[p, c]) for c in range(lcap)
        ]
        part += terms[0] + terms[1]
        middle = terms[0][HALF:] + pltpu.roll(terms[1][HALF:], HALF // 2, 0)
        packed = jnp.concatenate([terms[0][:HALF], middle, terms[1][:HALF]], axis=0)
        lsbuf[p, :PACKED] = packed.astype(BF16)
    for load in first_load:
        load.wait()
    for p in range(half):
        for c in range(cap):
            part += message(sbuf, p, c, send_block, send_target, send_count, send_w)
    for load in second_load:
        load.wait()
    for load in own_load:
        load.wait()
    for p in range(half, nd):
        for c in range(cap):
            part += message(sbuf, p, c, send_block, send_target, send_count, send_w)
    for b in range(blocks):
        term = product(own_src[0, b], own_w[b])
        part += term
        own_acc[b] = term

    sums = jnp.sum(part, axis=1, keepdims=True)
    same = row_id == lax.broadcasted_iota(jnp.int32, (ROWS, cells), 1)
    row = jnp.sum(jnp.where(same, sums, 0.0), axis=0, keepdims=True)
    trow[dev] = row

    def send(src, dst, k, who):
        pltpu.make_async_remote_copy(
            src_ref=src, dst_ref=dst, send_sem=send_sem.at[k], recv_sem=recv_sem.at[k], device_id=who, device_id_type=MESH
        ).start()

    pl.semaphore_wait(barrier, nd - 1 + lvl + lvl * (dev % 2) + jnp.where(is_far, 1, 0))

    @pl.loop(0, lvl)
    def _(p):
        pl.semaphore_signal(go_lvl, inc=1, device_id=at_lvl(p), device_id_type=MESH)

    def report(i):
        send(trow.at[dev], trow.at[dev], 0, at_dev(2 * i + 1))

    @pl.when(lvl != first_lvl)
    def _():
        send(trow.at[dev], every.at[lvl, dev], 4, {"dev": first_dev, "level": first_lvl})

    pl.loop(0, dev // 2)(report)
    pl.loop((dev + 1) // 2, nd // 2)(report)

    def pass_on(p):
        send(lsbuf.at[p, :PACKED], lrbuf.at[lvl, :PACKED], 1, at_lvl(p))
        send(places.at[lvl], places.at[lvl], 5, at_lvl(p))

    pl.loop(0, lvl)(pass_on)

    def wait_recv(buf, n, k):
        ref = buf.at[pl.ds(0, n - 1)]
        pltpu.make_async_copy(ref, ref, recv_sem.at[k]).wait()

    def wait_send(buf, n, k):
        ref = buf.at[pl.ds(0, n - 1)]
        pltpu.make_async_copy(ref, ref, send_sem.at[k]).wait()

    def total(ref, n):
        terms = [ref[i] for i in range(n)]
        while len(terms) > 1:
            half = len(terms) // 2
            terms = [a + b for a, b in zip(terms[:half], terms[half:])] + terms[2 * half :]
        return terms[0]

    def tell(p):
        send(urow.at[lvl], urow.at[lvl], 3, at_lvl(p))
        send(urow.at[lvl], urow.at[lvl], 3, at_partner(p))

    @pl.when(summing)
    def _():
        wait_recv(trow, nd, 0)
        urow[lvl] = total(trow, nd)
        pl.loop(jnp.where(dev == first_dev, jnp.minimum(1, lvl), 0), lvl)(tell)

        @pl.when(jnp.logical_and(dev == first_dev, lvl > 0))
        def _():
            send(urow.at[lvl], urow.at[lvl], 3, at_partner(0))

        send(urow.at[lvl], urow.at[lvl], 3, at_partner(lvl))

    def place(buf, acc, p, slots):
        for c in range(slots):
            got = buf[p, c * ROWS : (c + 1) * ROWS, :].astype(F32)
            target = jnp.broadcast_to(got[comp : comp + 1], (ROWS, cells))
            acc = [a + jnp.where(target == float(b), got, 0.0) for b, a in enumerate(acc)]
        return acc

    @other_devs
    def _(p):
        send(sbuf.at[p], rbuf.at[dev], 2, at_dev(p))

    @pl.when(lvl < nl - 1)
    def _():
        pl.semaphore_wait(go_lvl, nl - 1 - lvl)

    pl.loop(lvl + 1, nl)(pass_on)

    @pl.when(summing)
    def _():
        pl.loop(lvl + 1, nl)(tell)

    acc = [own_acc[b] for b in range(blocks)]
    wait_recv(rbuf, nd, 2)
    acc = lax.fori_loop(0, nd, lambda p, a: place(rbuf, a, p, cap), acc)
    wait_recv(lrbuf.at[:, :PACKED], nl, 1)
    wait_recv(places, nl, 5)
    at_level = lax.broadcasted_iota(jnp.int32, (lcap, nl), 1) == lvl
    for p in range(nl):
        target = jnp.sum(jnp.where(at_level, places[p].astype(F32), 0.0), axis=1, keepdims=True)
        targets[p] = jnp.broadcast_to(target, (lcap, cells))
    low = lax.broadcasted_iota(jnp.int32, (HALF, cells), 0) < HALF // 2
    heads = [a[:HALF] for a in acc]
    tails = [jnp.where(low, a[HALF:], 0.0) for a in acc]

    def unpack(p, state):
        heads, tails = state
        got = lrbuf[p, :PACKED].astype(F32)
        first, middle, second = got[:HALF], got[HALF : 2 * HALF], got[2 * HALF :]
        to_first = jnp.broadcast_to(targets[p, 0:1], (HALF, cells))
        to_second = jnp.broadcast_to(targets[p, 1:2], (HALF, cells))
        to_middle = jnp.where(low, to_first, to_second)
        heads = [
            h + jnp.where(to_first == float(b), first, 0.0) + jnp.where(to_second == float(b), second, 0.0)
            for b, h in enumerate(heads)
        ]
        tails = [t + jnp.where(to_middle == float(b), middle, 0.0) for b, t in enumerate(tails)]
        return heads, tails

    heads, tails = lax.fori_loop(0, nl, unpack, (heads, tails))
    for b in range(blocks):
        tail = tails[b] + pltpu.roll(tails[b], HALF // 2, 0)
        out_ref[pl.ds(b, comp, stride=blocks), :] = jnp.concatenate([heads[b], tail], axis=0)[:comp]
    wait_send(lsbuf.at[:, :PACKED], nl, 1)
    wait_send(places, nl, 5)
    wait_send(sbuf, nd, 2)

    def finish(rows):
        tot_ref[...] = (rows / (cells * blocks))[0, :comp]

    @pl.when(lvl != first_lvl)
    def _():
        wait_send(trow, 2, 4)

    @pl.when(jnp.logical_and(summing, jnp.logical_not(is_first)))
    def _():
        wait_send(trow, nd // 2, 0)

        @pl.when(dev == first_dev)
        def _():
            wait_send(trow, 2 * nl - 1, 3)

        @pl.when(dev != first_dev)
        def _():
            wait_send(trow, 2 * nl, 3)

        wait_recv(urow, nl, 3)
        finish(total(urow, nl))

    @pl.when(is_first)
    def _():
        wait_send(trow, nd // 2, 0)
        wait_send(trow, 2 * nl, 3)
        ref = every.at[pl.ds(1, nl - 1)]
        pltpu.make_async_copy(ref, ref, recv_sem.at[4]).wait()
        sums = [urow[0]]
        for l in range(1, nl):
            sums.append(total(every.at[l], nd))
        while len(sums) > 1:
            half = len(sums) // 2
            sums = [a + b for a, b in zip(sums[:half], sums[half:])] + sums[2 * half :]
        finish(sums[0])

    @pl.when(jnp.logical_not(summing))
    def _():
        wait_send(trow, nd // 2 + 1, 0)
        wait_recv(urow, nl + 1, 3)
        finish(total(urow, nl))


def deliver(blocks_in, totals_in, blocks_out, totals_out, sem):
    copies = [
        pltpu.make_async_copy(blocks_in, blocks_out, sem.at[0]),
        pltpu.make_async_copy(totals_in, totals_out, sem.at[1]),
    ]
    for copy in copies:
        copy.start()
    for copy in copies:
        copy.wait()


def solution(mesh):
    nd = mesh.shape["dev"]
    nl = mesh.shape["level"]

    def body(
        fields,
        own_src,
        own_weight,
        send_block,
        send_target,
        send_count,
        send_weight,
        left_block,
        left_target,
        left_count,
        left_weight,
    ):
        blocks, comp, cells = fields.shape[1:]
        cap = send_weight.shape[3]
        lcap = left_weight.shape[3]
        smem = functools.partial(pltpu.SMEM, dtype=jnp.int32)
        hbm = pl.BlockSpec(memory_space=pl.ANY)
        vmem = pl.BlockSpec(memory_space=pltpu.VMEM)
        dma = pltpu.SemaphoreType.DMA
        remapped, totals = pl.pallas_call(
            functools.partial(kernel, nd, nl, comp),
            out_shape=(
                pltpu.VMEM((comp * blocks, cells), F32),
                pltpu.VMEM((comp,), F32),
            ),
            in_specs=[hbm] * 11,
            out_specs=(vmem, vmem),
            scratch_shapes=[
                smem((1, blocks)),
                smem((cap, nd)),
                smem((cap, nd)),
                smem((1, nd)),
                smem((lcap, nl)),
                smem((1, nl)),
                pltpu.VMEM((comp * blocks, cells), F32),
                pltpu.VMEM((blocks, cells, cells), BF16),
                pltpu.VMEM((nd, cap, cells, cells), BF16),
                pltpu.VMEM((nl, lcap, cells, cells), BF16),
                dma((5,)),
                pltpu.VMEM((blocks + 1, ROWS, cells), BF16),
                pltpu.VMEM((blocks, ROWS, cells), F32),
                pltpu.VMEM((nd, cap * ROWS, cells), BF16),
                pltpu.VMEM((nd, cap * ROWS, cells), BF16),
                pltpu.VMEM((nl, lcap * ROWS, cells), BF16),
                pltpu.VMEM((nl, lcap * ROWS, cells), BF16),
                pltpu.VMEM((nd, 1, cells), F32),
                pltpu.VMEM((nl, 1, cells), F32),
                pltpu.VMEM((nl, nd, 1, cells), F32),
                pltpu.VMEM((nl, lcap, nl), jnp.int32),
                pltpu.VMEM((nl, lcap, cells), F32),
                pltpu.SemaphoreType.REGULAR,
                dma((6,)),
                dma((6,)),
            ],
            compiler_params=pltpu.CompilerParams(collective_id=0, has_side_effects=True),
        )(
            own_src,
            send_block[0, 0].T,
            send_target[0, 0].T,
            send_count[0],
            left_block[0, 0].T,
            left_target[0, 0].T,
            left_count[0],
            fields[0].transpose(1, 0, 2).reshape(comp * blocks, cells),
            own_weight[0],
            send_weight[0, 0],
            left_weight[0, 0],
        )
        remapped, totals = pl.pallas_call(
            deliver,
            out_shape=(
                jax.ShapeDtypeStruct((comp * blocks, cells), F32),
                jax.ShapeDtypeStruct((comp,), F32),
            ),
            in_specs=[vmem] * 2,
            out_specs=(hbm, hbm),
            scratch_shapes=[dma((2,))],
            compiler_params=pltpu.CompilerParams(vmem_limit_bytes=1 << 20),
        )(pltpu.with_memory_space_constraint(remapped, pltpu.VMEM), pltpu.with_memory_space_constraint(totals, pltpu.VMEM))
        remapped = remapped.reshape(comp, blocks, cells).transpose(1, 0, 2)
        return remapped[None], totals

    in_specs = (
        P("level", "dev", None, None),
        P("level", "dev"),
        P("level", "dev", None, None),
        P("level", "dev", None, None),
        P("level", "dev", None, None),
        P("level", "dev", None),
        P("level", "dev", None, None, None, None),
        P("level", "dev", None, None),
        P("level", "dev", None, None),
        P("level", "dev", None),
        P("level", "dev", None, None, None, None),
    )
    out_specs = (P("level", "dev", None, None), P())
    return jax.shard_map(body, mesh=mesh, in_specs=in_specs, out_specs=out_specs, check_vma=False)
```

```python
import functools

import jax
import jax.numpy as jnp
from jax import lax
from jax.experimental import pallas as pl
from jax.experimental.pallas import tpu as pltpu
from jax.sharding import PartitionSpec as P

MESH = pl.DeviceIdType.MESH
F32 = jnp.float32
BF16 = jnp.bfloat16
ROWS = 16
HALF = 8
PACKED = 24
PIECES = 4


def kernel(
    nd,
    nl,
    comp,
    own_src_hbm,
    send_block_hbm,
    send_target_hbm,
    send_count_hbm,
    left_block_hbm,
    left_target_hbm,
    left_count_hbm,
    fields_hbm,
    own_hbm,
    send_hbm,
    left_hbm,
    out_ref,
    tot_ref,
    own_src,
    send_block,
    send_target,
    send_count,
    left_block,
    left_count,
    fields,
    own_w,
    send_w,
    left_w,
    load_sem,
    rounded,
    own_acc,
    sbuf,
    rbuf,
    lsbuf,
    lrbuf,
    trow,
    urow,
    every,
    places,
    targets,
    go_lvl,
    send_sem,
    recv_sem,
):
    dev = lax.axis_index("dev")
    lvl = lax.axis_index("level")
    blocks, cells = own_w.shape[:2]
    cap = send_w.shape[1]
    lcap = left_w.shape[1]

    tables = [
        (left_block_hbm, left_block),
        (left_count_hbm, left_count),
        (send_block_hbm, send_block),
        (send_count_hbm, send_count),
        (send_target_hbm, send_target),
        (own_src_hbm, own_src),
        (fields_hbm, fields),
        (left_target_hbm, places.at[lvl]),
    ]
    table_loads = [pltpu.make_async_copy(src, dst, load_sem.at[0]) for src, dst in tables]
    half = nd // 2

    def pieces(src, dst, lo, hi, n, k):
        size = (hi - lo) // n
        return [
            pltpu.make_async_copy(
                src.at[lo + i * size : lo + (i + 1) * size], dst.at[lo + i * size : lo + (i + 1) * size], load_sem.at[k]
            )
            for i in range(n)
        ]

    left_load = pieces(left_hbm, left_w, 0, nl, PIECES, 1)
    first_load = pieces(send_hbm, send_w, 0, half, PIECES, 2)
    second_load = pieces(send_hbm, send_w, half, nd, PIECES, 3)
    own_load = pieces(own_hbm, own_w, 0, blocks, PIECES // 2, 3)
    for load in [*table_loads, *left_load, *first_load, *second_load, *own_load]:
        load.start()

    barrier = pltpu.get_barrier_semaphore()

    def at_dev(p):
        return {"dev": p, "level": lvl}

    def at_lvl(p):
        return {"dev": dev, "level": p}

    def other_devs(step):
        pl.loop(0, dev)(step)
        pl.loop(dev + 1, nd)(step)

    @other_devs
    def _(p):
        pl.semaphore_signal(barrier, inc=1, device_id=at_dev(p), device_id_type=MESH)

    summing = dev % 2 == 1
    partner = dev + 1 - 2 * (dev % 2)

    def at_partner(p):
        return {"dev": partner, "level": p}

    @pl.loop(lvl + 1, nl)
    def _(p):
        pl.semaphore_signal(barrier, inc=1, device_id=at_lvl(p), device_id_type=MESH)

    @pl.when(jnp.logical_not(summing))
    def _():
        @pl.loop(lvl + 1, nl)
        def _(p):
            pl.semaphore_signal(barrier, inc=1, device_id=at_partner(p), device_id_type=MESH)

    first_dev, first_lvl = 1, 0
    is_first = jnp.logical_and(dev == first_dev, lvl == first_lvl)
    is_far = jnp.logical_and(dev != first_dev, lvl != first_lvl)

    @pl.when(is_first)
    def _():
        @pl.loop(1, nl)
        def _(l):
            def greet(p):
                pl.semaphore_signal(barrier, inc=1, device_id={"dev": p, "level": l}, device_id_type=MESH)

            pl.loop(0, first_dev)(greet)
            pl.loop(first_dev + 1, nd)(greet)

    zero = jnp.zeros((2 * ROWS, cells), BF16)
    rbuf[dev] = zero
    lrbuf[lvl, :PACKED] = zero[:PACKED]

    for load in table_loads:
        load.wait()

    pad = jnp.zeros((ROWS - comp, cells), F32)
    for b in range(blocks):
        block = fields[pl.ds(b, comp, stride=blocks), :]
        rounded[b] = jnp.concatenate([block, pad], axis=0).astype(BF16)
    rounded[blocks] = jnp.zeros((ROWS, cells), BF16)

    row_id = lax.broadcasted_iota(jnp.int32, (ROWS, cells), 0)

    def product(index, weight):
        return jnp.dot(rounded[index], weight, preferred_element_type=F32)

    def message(buf, p, c, slot_block, slot_target, slot_count, weights):
        index = jnp.where(c < slot_count[0, p], slot_block[c, p], blocks)
        term = product(index, weights[p, c])
        target = slot_target[c, p].astype(F32)
        buf[p, c * ROWS : (c + 1) * ROWS, :] = jnp.where(row_id == comp, target, term).astype(BF16)
        return term

    part = jnp.zeros((ROWS, cells), F32)
    for load in left_load:
        load.wait()
    for p in range(nl):
        terms = [
            product(jnp.where(c < left_count[0, p], left_block[c, p], blocks), left_w[p, c]) for c in range(lcap)
        ]
        part += terms[0] + terms[1]
        middle = terms[0][HALF:] + pltpu.roll(terms[1][HALF:], HALF // 2, 0)
        packed = jnp.concatenate([terms[0][:HALF], middle, terms[1][:HALF]], axis=0)
        lsbuf[p, :PACKED] = packed.astype(BF16)
    for load in first_load:
        load.wait()
    for p in range(half):
        for c in range(cap):
            part += message(sbuf, p, c, send_block, send_target, send_count, send_w)
    for load in second_load:
        load.wait()
    for load in own_load:
        load.wait()
    for p in range(half, nd):
        for c in range(cap):
            part += message(sbuf, p, c, send_block, send_target, send_count, send_w)
    for b in range(blocks):
        term = product(own_src[0, b], own_w[b])
        part += term
        own_acc[b] = term

    sums = jnp.sum(part, axis=1, keepdims=True)
    same = row_id == lax.broadcasted_iota(jnp.int32, (ROWS, cells), 1)
    row = jnp.sum(jnp.where(same, sums, 0.0), axis=0, keepdims=True)
    trow[dev] = row

    def send(src, dst, k, who):
        pltpu.make_async_remote_copy(
            src_ref=src, dst_ref=dst, send_sem=send_sem, recv_sem=recv_sem.at[k], device_id=who, device_id_type=MESH
        ).start()

    pl.semaphore_wait(barrier, nd - 1 + lvl + lvl * (dev % 2) + jnp.where(is_far, 1, 0))

    @pl.when(lvl != first_lvl)
    def _():
        send(trow.at[dev], every.at[lvl, dev], 4, {"dev": first_dev, "level": first_lvl})

    @pl.loop(0, lvl)
    def _(p):
        pl.semaphore_signal(go_lvl, inc=1, device_id=at_lvl(p), device_id_type=MESH)

    def report(i):
        send(trow.at[dev], trow.at[dev], 0, at_dev(2 * i + 1))

    pl.loop(0, dev // 2)(report)
    pl.loop((dev + 1) // 2, nd // 2)(report)

    def pass_on(p):
        send(lsbuf.at[p, :PACKED], lrbuf.at[lvl, :PACKED], 1, at_lvl(p))
        send(places.at[lvl], places.at[lvl], 5, at_lvl(p))

    pl.loop(0, lvl)(pass_on)

    def wait_recv(buf, n, k):
        ref = buf.at[pl.ds(0, n - 1)]
        pltpu.make_async_copy(ref, ref, recv_sem.at[k]).wait()

    def wait_send(buf, n):
        ref = buf.at[pl.ds(0, n - 1)]
        pltpu.make_async_copy(ref, ref, send_sem).wait()

    def total(ref, n):
        terms = [ref[i] for i in range(n)]
        while len(terms) > 1:
            half = len(terms) // 2
            terms = [a + b for a, b in zip(terms[:half], terms[half:])] + terms[2 * half :]
        return terms[0]

    def tell(p):
        send(urow.at[lvl], urow.at[lvl], 3, at_lvl(p))
        send(urow.at[lvl], urow.at[lvl], 3, at_partner(p))

    @pl.when(summing)
    def _():
        wait_recv(trow, nd, 0)
        urow[lvl] = total(trow, nd)
        pl.loop(jnp.where(dev == first_dev, jnp.minimum(1, lvl), 0), lvl)(tell)

        @pl.when(jnp.logical_and(dev == first_dev, lvl > 0))
        def _():
            send(urow.at[lvl], urow.at[lvl], 3, at_partner(0))

        send(urow.at[lvl], urow.at[lvl], 3, at_partner(lvl))

    def place(buf, acc, p, slots):
        for c in range(slots):
            got = buf[p, c * ROWS : (c + 1) * ROWS, :].astype(F32)
            target = jnp.broadcast_to(got[comp : comp + 1], (ROWS, cells))
            acc = [a + jnp.where(target == float(b), got, 0.0) for b, a in enumerate(acc)]
        return acc

    @other_devs
    def _(p):
        send(sbuf.at[p], rbuf.at[dev], 2, at_dev(p))

    @pl.when(lvl < nl - 1)
    def _():
        pl.semaphore_wait(go_lvl, nl - 1 - lvl)

    middle = jnp.minimum(lvl + nl // 2, nl - 1)

    @pl.loop(lvl + 1, nl)
    def _(q):
        pass_on(jnp.where(q <= middle, middle + lvl + 1 - q, q))

    @pl.when(summing)
    def _():
        pl.loop(lvl + 1, nl)(tell)

    acc = [own_acc[b] for b in range(blocks)]
    wait_recv(rbuf, nd, 2)
    acc = lax.fori_loop(0, nd, lambda p, a: place(rbuf, a, p, cap), acc)
    wait_recv(lrbuf.at[:, :PACKED], nl, 1)
    wait_recv(places, nl, 5)
    at_level = lax.broadcasted_iota(jnp.int32, (lcap, nl), 1) == lvl
    for p in range(nl):
        target = jnp.sum(jnp.where(at_level, places[p].astype(F32), 0.0), axis=1, keepdims=True)
        targets[p] = jnp.broadcast_to(target, (lcap, cells))
    low = lax.broadcasted_iota(jnp.int32, (HALF, cells), 0) < HALF // 2
    heads = [a[:HALF] for a in acc]
    tails = [jnp.where(low, a[HALF:], 0.0) for a in acc]

    def unpack(p, state):
        heads, tails = state
        got = lrbuf[p, :PACKED].astype(F32)
        first, middle, second = got[:HALF], got[HALF : 2 * HALF], got[2 * HALF :]
        to_first = jnp.broadcast_to(targets[p, 0:1], (HALF, cells))
        to_second = jnp.broadcast_to(targets[p, 1:2], (HALF, cells))
        to_middle = jnp.where(low, to_first, to_second)
        heads = [
            h + jnp.where(to_first == float(b), first, 0.0) + jnp.where(to_second == float(b), second, 0.0)
            for b, h in enumerate(heads)
        ]
        tails = [t + jnp.where(to_middle == float(b), middle, 0.0) for b, t in enumerate(tails)]
        return heads, tails

    heads, tails = lax.fori_loop(0, nl, unpack, (heads, tails))
    for b in range(blocks):
        tail = tails[b] + pltpu.roll(tails[b], HALF // 2, 0)
        out_ref[pl.ds(b, comp, stride=blocks), :] = jnp.concatenate([heads[b], tail], axis=0)[:comp]
    wait_send(lsbuf.at[:, :PACKED], nl)
    wait_send(places, nl)
    wait_send(sbuf, nd)

    def finish(rows):
        tot_ref[...] = (rows / (cells * blocks))[0, :comp]

    @pl.when(lvl != first_lvl)
    def _():
        wait_send(trow, 2)

    @pl.when(jnp.logical_and(summing, jnp.logical_not(is_first)))
    def _():
        wait_send(trow, nd // 2)

        @pl.when(dev == first_dev)
        def _():
            wait_send(trow, 2 * nl - 1)

        @pl.when(dev != first_dev)
        def _():
            wait_send(trow, 2 * nl)

        wait_recv(urow, nl, 3)
        finish(total(urow, nl))

    @pl.when(is_first)
    def _():
        wait_send(trow, nd // 2)
        wait_send(trow, 2 * nl)
        ref = every.at[pl.ds(1, nl - 1)]
        pltpu.make_async_copy(ref, ref, recv_sem.at[4]).wait()
        sums = [urow[0]]
        for l in range(1, nl):
            sums.append(total(every.at[l], nd))
        while len(sums) > 1:
            half = len(sums) // 2
            sums = [a + b for a, b in zip(sums[:half], sums[half:])] + sums[2 * half :]
        finish(sums[0])

    @pl.when(jnp.logical_not(summing))
    def _():
        wait_send(trow, nd // 2 + 1)
        wait_recv(urow, nl + 1, 3)
        finish(total(urow, nl))


def deliver(blocks_in, totals_in, blocks_out, totals_out, sem):
    copies = [
        pltpu.make_async_copy(blocks_in, blocks_out, sem.at[0]),
        pltpu.make_async_copy(totals_in, totals_out, sem.at[1]),
    ]
    for copy in copies:
        copy.start()
    for copy in copies:
        copy.wait()


def solution(mesh):
    nd = mesh.shape["dev"]
    nl = mesh.shape["level"]

    def body(
        fields,
        own_src,
        own_weight,
        send_block,
        send_target,
        send_count,
        send_weight,
        left_block,
        left_target,
        left_count,
        left_weight,
    ):
        blocks, comp, cells = fields.shape[1:]
        cap = send_weight.shape[3]
        lcap = left_weight.shape[3]
        smem = functools.partial(pltpu.SMEM, dtype=jnp.int32)
        hbm = pl.BlockSpec(memory_space=pl.ANY)
        vmem = pl.BlockSpec(memory_space=pltpu.VMEM)
        dma = pltpu.SemaphoreType.DMA
        remapped, totals = pl.pallas_call(
            functools.partial(kernel, nd, nl, comp),
            out_shape=(
                pltpu.VMEM((comp * blocks, cells), F32),
                pltpu.VMEM((comp,), F32),
            ),
            in_specs=[hbm] * 11,
            out_specs=(vmem, vmem),
            scratch_shapes=[
                smem((1, blocks)),
                smem((cap, nd)),
                smem((cap, nd)),
                smem((1, nd)),
                smem((lcap, nl)),
                smem((1, nl)),
                pltpu.VMEM((comp * blocks, cells), F32),
                pltpu.VMEM((blocks, cells, cells), BF16),
                pltpu.VMEM((nd, cap, cells, cells), BF16),
                pltpu.VMEM((nl, lcap, cells, cells), BF16),
                dma((4,)),
                pltpu.VMEM((blocks + 1, ROWS, cells), BF16),
                pltpu.VMEM((blocks, ROWS, cells), F32),
                pltpu.VMEM((nd, cap * ROWS, cells), BF16),
                pltpu.VMEM((nd, cap * ROWS, cells), BF16),
                pltpu.VMEM((nl, lcap * ROWS, cells), BF16),
                pltpu.VMEM((nl, lcap * ROWS, cells), BF16),
                pltpu.VMEM((nd, 1, cells), F32),
                pltpu.VMEM((nl, 1, cells), F32),
                pltpu.VMEM((nl, nd, 1, cells), F32),
                pltpu.VMEM((nl, lcap, nl), jnp.int32),
                pltpu.VMEM((nl, lcap, cells), F32),
                pltpu.SemaphoreType.REGULAR,
                pltpu.SemaphoreType.DMA,
                dma((6,)),
            ],
            compiler_params=pltpu.CompilerParams(collective_id=0, has_side_effects=True),
        )(
            own_src,
            send_block[0, 0].T,
            send_target[0, 0].T,
            send_count[0],
            left_block[0, 0].T,
            left_target[0, 0].T,
            left_count[0],
            fields[0].transpose(1, 0, 2).reshape(comp * blocks, cells),
            own_weight[0],
            send_weight[0, 0],
            left_weight[0, 0],
        )
        remapped, totals = pl.pallas_call(
            deliver,
            out_shape=(
                jax.ShapeDtypeStruct((comp * blocks, cells), F32),
                jax.ShapeDtypeStruct((comp,), F32),
            ),
            in_specs=[vmem] * 2,
            out_specs=(hbm, hbm),
            scratch_shapes=[dma((2,))],
            compiler_params=pltpu.CompilerParams(vmem_limit_bytes=1 << 20),
        )(pltpu.with_memory_space_constraint(remapped, pltpu.VMEM), pltpu.with_memory_space_constraint(totals, pltpu.VMEM))
        remapped = remapped.reshape(comp, blocks, cells).transpose(1, 0, 2)
        return remapped[None], totals

    in_specs = (
        P("level", "dev", None, None),
        P("level", "dev"),
        P("level", "dev", None, None),
        P("level", "dev", None, None),
        P("level", "dev", None, None),
        P("level", "dev", None),
        P("level", "dev", None, None, None, None),
        P("level", "dev", None, None),
        P("level", "dev", None, None),
        P("level", "dev", None),
        P("level", "dev", None, None, None, None),
    )
    out_specs = (P("level", "dev", None, None), P())
    return jax.shard_map(body, mesh=mesh, in_specs=in_specs, out_specs=out_specs, check_vma=False)
```
